32 devices in a mesh: coil: 8 (over y, x, core), kz: 4 (over z).
Axes of the slice: x: 2, y: 2, z: 4, core: 2. Of those that a mesh axis runs over, the one named last changes fastest.
Arguments:
- kdata: bfloat16 [2, 64, 8, 256, 512], P(None, 'kz', 'coil'), may hold values from -6 to 6
- spoke_angle: int32 [256], replicated, may hold values from 0 to 63
- spoke_count: int32 [64], P('kz'), may hold values from 128 to 256
- block_index: int32 [64, 4], replicated, may hold values from 0 to 511
- interp: bfloat16 [64, 4, 128, 128], replicated, may hold values from -0.5 to 0.5
- sens_maps: bfloat16 [2, 8, 256, 256], P(None, 'coil'), may hold values from -5 to 5
Outputs:
- image: float32 [2, 64, 256, 256], P(None, 'kz', 'coil')
The draws below stay inside these ranges and needn't reach their ends.
Inputs may be any that keep to these rules, and one draw needn't show every extreme that they name: Partition p uses its first spoke_count[p] spokes. `block_index`: several segments may hit the same grid block.
All inputs are finite; a program needn't handle non-finite values.
Results may differ from the reference program's by a relative error of at most 0.0059.
Values sent between devices are 32-bit elements; how exact they have to be, the bound alone decides.
No kernel may reach another device: no remote copies, remote signals or barrier semaphores. Data moves between devices by JAX's collectives and lax.ppermute only.
A program may use at most 128 MiB of HBM per device.

```python
import jax
import jax.numpy as jnp
from jax import lax

N = 256
SAMPLES = 512
SEG_LEN = 128
SEGS = 4
BLOCKS = 512
SPOKES = 256
ANGLES = 64
KZ = 64
COILS = 8


def place_ends(values, key, smallest, largest):
    spot = [jax.random.randint(jax.random.fold_in(key, axis), (), 0, length) for axis, length in enumerate(values.shape)]
    main_axis = values.shape.index(max(values.shape))
    next_to = spot[:main_axis] + [(spot[main_axis] + 1) % values.shape[main_axis]] + spot[main_axis + 1:]
    return values.at[tuple(spot)].set(smallest).at[tuple(next_to)].set(largest)


def level_of(stream_key, dims, cuts, smallest, largest):
    def one(dim, blocks):
        steps = jax.random.uniform(jax.random.fold_in(jax.random.fold_in(stream_key, 6), dim), (blocks,), jnp.float32, smallest / len(cuts), largest / len(cuts))
        return jnp.repeat(jnp.exp(steps), dims[dim] // blocks).reshape((-1,) + (1,) * (len(dims) - dim - 1))

    factor_of = one(*cuts[0])
    for cut in cuts[1:]:
        factor_of = factor_of * one(*cut)
    return factor_of


def centred(rng, shape, width, limit, cuts=(), kind=jnp.bfloat16):
    values = width * jax.random.normal(rng, shape, jnp.float32)
    if cuts:
        values = values * level_of(rng, shape, cuts, -0.22, 0.18)
    return jnp.clip(values, -limit, limit).astype(kind)


def setup_inputs(seed: int = 0) -> dict:
    arg_keys = jax.random.split(jax.random.key(seed), 7)
    return {
        "kdata": centred(arg_keys[0], (2, KZ, COILS, SPOKES, SAMPLES), 1.0, 6.0, ((1, 4), (2, 8))),
        "spoke_angle": place_ends(jax.random.randint(arg_keys[1], (SPOKES,), 0, ANGLES), jax.random.fold_in(arg_keys[1], 1), 0, ANGLES - 1).astype(jnp.int32),
        "spoke_count": place_ends(jax.random.randint(arg_keys[2], (KZ,), SPOKES // 2, SPOKES + 1), jax.random.fold_in(arg_keys[2], 1), SPOKES // 2, SPOKES).astype(jnp.int32),
        "block_index": place_ends(jax.random.randint(arg_keys[3], (ANGLES, SEGS), 0, BLOCKS), jax.random.fold_in(arg_keys[3], 1), 0, BLOCKS - 1).astype(jnp.int32),
        "interp": centred(arg_keys[4], (ANGLES, SEGS, SEG_LEN, SEG_LEN), SEG_LEN ** -0.5, 0.5),
        "sens_maps": centred(arg_keys[5], (2, COILS, N, N), (COILS ** -0.5), 5.0, ((1, 8),)),
    }


def dft_tables(length, dtype):
    index = jnp.arange(length, dtype=jnp.int32)
    product = index[:, None] * index[None, :] % length
    phase = product.astype(jnp.float32) * (2.0 * jnp.pi / length)
    scale = 1.0 / jnp.sqrt(jnp.float32(length))
    return ((jnp.cos(phase) * scale).astype(dtype), (jnp.sin(phase) * scale).astype(dtype))

def spoke_weights(spoke_count, spoke_angle, angles, spokes):
    position = jnp.arange(spokes, dtype=jnp.int32)
    used = position[None, :] < spoke_count[:, None]
    match = spoke_angle[:, None] == jnp.arange(angles, dtype=jnp.int32)[None, :]
    return (used[:, :, None] & match[None, :, :]).astype(jnp.bfloat16)

def coil_image(data, weights, interp, block_index, cos_t, sin_t):
    f32 = jnp.float32
    binned = jnp.einsum('rpsn,psa->rpan', data.astype(f32), weights.astype(f32)).astype(jnp.bfloat16)
    rdim, pdim, adim, mdim = binned.shape
    seg = interp.shape[2]
    gdim = mdim // seg
    side = cos_t.shape[0]
    pieces = binned.reshape(rdim, pdim, adim, gdim, seg)
    contrib = jnp.einsum('rpagj,agjt->rpagt', pieces.astype(f32), interp.astype(f32))
    flat = jnp.zeros((rdim, pdim, side * side // seg, seg), f32)
    flat = flat.at[:, :, block_index.reshape(-1)].add(contrib.reshape(rdim, pdim, adim * gdim, seg))
    grid = flat.reshape(rdim, pdim, side, side).astype(jnp.bfloat16)
    cosf = cos_t.astype(f32)
    sinf = sin_t.astype(f32)
    grid_re = grid[0].astype(f32)
    grid_im = grid[1].astype(f32)
    half_re = jnp.einsum('ky,pyx->pkx', cosf, grid_re) + jnp.einsum('ky,pyx->pkx', sinf, grid_im)
    half_im = jnp.einsum('ky,pyx->pkx', cosf, grid_im) - jnp.einsum('ky,pyx->pkx', sinf, grid_re)
    half_re = half_re.astype(jnp.bfloat16).astype(f32)
    half_im = half_im.astype(jnp.bfloat16).astype(f32)
    out_re = jnp.einsum('pkx,mx->pkm', half_re, cosf) + jnp.einsum('pkx,mx->pkm', half_im, sinf)
    out_im = jnp.einsum('pkx,mx->pkm', half_im, cosf) - jnp.einsum('pkx,mx->pkm', half_re, sinf)
    return jnp.stack([out_re, out_im])

def conj_product(sens, image):
    real_part = sens[0] * image[0] + sens[1] * image[1]
    imag_part = sens[0] * image[1] - sens[1] * image[0]
    return jnp.stack([real_part, imag_part])

def reference(kdata, spoke_angle, spoke_count, block_index, interp, sens_maps):
    cos_t, sin_t = dft_tables(N, jnp.bfloat16)
    weights = spoke_weights(spoke_count, spoke_angle, ANGLES, SPOKES)

    def per_coil(total, coil_id):
        data = lax.dynamic_index_in_dim(kdata, coil_id, 2, keepdims=False)
        image_c = coil_image(data, weights, interp, block_index, cos_t, sin_t)
        sens = lax.dynamic_index_in_dim(sens_maps, coil_id, 1, keepdims=False).astype(jnp.float32)
        return (total + conj_product(sens[:, None], image_c), None)
    start = jnp.zeros((2, KZ, N, N), jnp.float32)
    combined, unused = lax.scan(per_coil, start, jnp.arange(COILS, dtype=jnp.int32))
    cos_z, sin_z = dft_tables(KZ, jnp.float32)
    high = lax.Precision.HIGHEST
    image_re = jnp.einsum('zk,kyx->zyx', cos_z, combined[0], precision=high) + jnp.einsum('zk,kyx->zyx', sin_z, combined[1], precision=high)
    image_im = jnp.einsum('zk,kyx->zyx', cos_z, combined[1], precision=high) - jnp.einsum('zk,kyx->zyx', sin_z, combined[0], precision=high)
    return jnp.stack([image_re, image_im])
```

```python
import jax
import jax.numpy as jnp
import numpy as np
from jax import lax
from jax.experimental import pallas as pl
from jax.experimental.pallas import tpu as pltpu
from jax.sharding import PartitionSpec as P


def host_tables(length, dtype):
    index = np.arange(length, dtype=np.int32)
    product = index[:, None] * index[None, :] % length
    phase = product.astype(np.float32) * np.float32(2.0 * np.pi / length)
    scale = np.float32(1.0) / np.sqrt(np.float32(length))
    return ((np.cos(phase) * scale).astype(dtype), (np.sin(phase) * scale).astype(dtype))


def grid_kernel(
    count_ref, bidx_ref, rows_ref, angle_ref, cos_ref, sin_ref, sens_ref, data_ref, interp_hbm,
    half_ref, sensp_ref,
    bin_ref, grid_ref, m1_ref, interp_ref, sem,
):
    f32, bf16 = jnp.float32, jnp.bfloat16
    step = pl.program_id(0)
    parts = pl.num_programs(0) // 2
    angles, segs = bidx_ref.shape
    seg = interp_ref.shape[1]
    side = cos_ref.shape[0]
    spokes = angle_ref.shape[1]
    lines = 2 * bin_ref.shape[1] // (2 * angles)
    nblocks = grid_ref.shape[0] // lines
    per_row = side // seg
    nparts = lines // 2

    @pl.when(step == 0)
    def _():
        pltpu.make_async_copy(interp_hbm, interp_ref, sem).start()
        pick = (lax.broadcasted_iota(jnp.int32, (side, side), 1) == rows_ref[...]).astype(bf16)
        pc = jnp.dot(pick, cos_ref[...], preferred_element_type=f32)
        ps = jnp.dot(pick, sin_ref[...], preferred_element_type=f32)
        m1_ref[:side, :side] = pc.astype(bf16)
        m1_ref[:side, side:] = ps.astype(bf16)
        m1_ref[side:, :side] = (-ps).astype(bf16)
        m1_ref[side:, side:] = pc.astype(bf16)
        for r in range(2):
            sensp_ref[r] = jnp.dot(pick, sens_ref[r], preferred_element_type=f32)

    @pl.when(step < parts)
    def _():
        zrows = grid_ref.shape[0] // nparts
        grid_ref[pl.ds(step * zrows, zrows), :] = jnp.zeros((zrows, seg), f32)
        a_iota = lax.broadcasted_iota(jnp.int32, (angles, spokes), 0)
        s_iota = lax.broadcasted_iota(jnp.int32, (angles, spokes), 1)
        keep = (a_iota == angle_ref[...]) & (s_iota < count_ref[step])
        wt = jnp.where(keep, 1.0, 0.0).astype(bf16)
        for r in range(2):
            b = jnp.dot(wt, data_ref[r, 0], preferred_element_type=f32)
            b = b.astype(bf16).astype(f32)
            for g in range(segs):
                bin_ref[g, pl.ds((r * nparts + step) * angles, angles), :] = b[:, g * seg:(g + 1) * seg]

    @pl.when(step == parts)
    def _():
        pltpu.make_async_copy(interp_hbm, interp_ref, sem).wait()
        unroll = 4 if angles % 4 == 0 else 1

        def body(i, carry):
            res = []
            for u in range(unroll):
                a = i * unroll + u
                for g in range(segs):
                    lhs = bin_ref[g, pl.ds(a, lines, stride=angles), :].astype(bf16)
                    res.append((bidx_ref[a, g], jnp.dot(lhs, interp_ref[a * segs + g], preferred_element_type=f32)))
            for b, v in res:
                at = pl.ds(pl.multiple_of(b * lines, lines), lines)
                grid_ref[at, :] = grid_ref[at, :] + v
            return carry

        lax.fori_loop(0, angles // unroll, body, 0)

    @pl.when(step >= parts)
    def _():
        p = step - parts
        stacked = jnp.concatenate(
            [
                jnp.concatenate(
                    [
                        grid_ref[pl.ds(h * lines + r * nparts + p, side, stride=per_row * lines), :].astype(bf16)
                        for h in range(per_row)
                    ],
                    axis=1,
                )
                for r in range(2)
            ],
            axis=0,
        )
        half = jnp.dot(m1_ref[...], stacked, preferred_element_type=f32).astype(bf16)
        half_ref[0, :, :side] = half[:side]
        half_ref[0, :, side:] = half[side:]


def image_kernel(half_ref, m2_ref, sens_ref, send_ref, keep_ref):
    pp, side, depth = half_ref.shape
    width = m2_ref.shape[1] // 2
    pieces = keep_ref.shape[0]
    sub = keep_ref.shape[3]
    out = jnp.dot(half_ref[...].reshape(pp * side, depth), m2_ref[...], preferred_element_type=jnp.float32)
    for q in range(pp):
        re = out[q * side:(q + 1) * side, :width]
        im = out[q * side:(q + 1) * side, width:]
        w = (sens_ref[0] * re + sens_ref[1] * im, sens_ref[0] * im - sens_ref[1] * re)
        for r in range(2):
            keep_ref[:, r, q] = w[r][:side // 2].reshape(pieces, sub, width)
            send_ref[:, r, q] = w[r][side // 2:].reshape(pieces, sub, width)


def kz_kernel(z_ref, *refs):
    n = len(refs) // 2
    ins, outs = refs[:n], refs[n:]
    rows, width = ins[0].shape
    sub = 8
    cnt = rows // (2 * sub)
    x = jnp.concatenate(
        [
            jnp.concatenate(
                [ins[s][pl.ds(r * cnt * sub + i, cnt, stride=sub), :] for s in range(n) for r in range(2)], axis=0
            )
            for i in range(sub)
        ],
        axis=1,
    )
    y = jnp.dot(z_ref[...], x, preferred_element_type=jnp.float32, precision=lax.Precision.HIGHEST)
    for s in range(n):
        for r in range(2):
            for i in range(sub):
                outs[s][pl.ds(r * cnt * sub + i, cnt, stride=sub), :] = y[
                    (s * 2 + r) * cnt:(s * 2 + r + 1) * cnt, i * width:(i + 1) * width
                ]


def place_kernel(me_ref, *refs):
    out_ref = refs[-1]
    ins = refs[:-1]
    n = out_ref.shape[2] // ins[0].shape[2]
    width = ins[0].shape[3]
    sub = ins[0].shape[2]
    for j in range(len(ins) // n):
        for s in range(n):
            at = pl.multiple_of((me_ref[0] ^ s) * sub, sub)
            out_ref[:, :, pl.ds(at, sub), j * width:(j + 1) * width] = ins[j * n + s][...]


def swap(x, axis, bit):
    n = lax.axis_size(axis)
    return lax.ppermute(x, axis, [(i, i ^ bit) for i in range(n)])


def piece_order():
    order = []
    for relc in range(2):
        order += [(relc, 1, ry, rd) for ry in range(2) for rd in (0, 1)]
        order += [(relc, 0, ry, rd) for ry in range(2) for rd in (0, 1)]
        order += [(relc, rx, 1, rd) for rx in range(2) for rd in (2, 3)]
        order += [(relc, rx, 0, rd) for rx in range(2) for rd in (2, 3)]
    coil_rel = np.array([c + 2 * x + 4 * y for c, x, y, d in order], np.int32)
    kz_rel = np.array([d for c, x, y, d in order], np.int32)
    return coil_rel, kz_rel


def fast_device(kdata, spoke_angle, spoke_count, block_index, interp, sens_maps):
    f32, bf16 = jnp.float32, jnp.bfloat16
    _, parts, _, spokes, samples = kdata.shape
    side = sens_maps.shape[2]
    angles, segs, seg, _ = interp.shape
    groups = lax.axis_size("kz")
    mine_c = lax.axis_index("coil")
    mine_d = lax.axis_index("kz")
    sub = side // (lax.axis_size("coil") * groups)
    coil_rel, kz_rel = piece_order()
    starts = (mine_c ^ coil_rel) * (sub * groups) + (mine_d ^ kz_rel) * sub
    rows = (starts[:, None] + np.arange(sub, dtype=np.int32)[None, :]).reshape(side, 1)
    cos_h, sin_h = host_tables(side, np.float32)
    cos_t, sin_t = jnp.asarray(cos_h).astype(bf16), jnp.asarray(sin_h).astype(bf16)
    lines = 2 * parts
    smem = pl.BlockSpec(memory_space=pltpu.SMEM)
    whole = lambda shape: pl.BlockSpec(shape, lambda i: (0,) * len(shape))
    half, sens_p = pl.pallas_call(
        grid_kernel,
        grid=(2 * parts,),
        in_specs=[
            smem, smem, whole((side, 1)), whole((1, spokes)), whole((side, side)), whole((side, side)),
            whole((2, side, side)),
            pl.BlockSpec((2, 1, spokes, samples), lambda i: (0, jnp.minimum(i, parts - 1), 0, 0)),
            pl.BlockSpec(memory_space=pl.ANY),
        ],
        out_specs=[
            pl.BlockSpec((1, side, 2 * side), lambda i: (jnp.maximum(i - parts, 0), 0, 0)),
            whole((2, side, side)),
        ],
        out_shape=[
            jax.ShapeDtypeStruct((parts, side, 2 * side), bf16),
            jax.ShapeDtypeStruct((2, side, side), f32),
        ],
        scratch_shapes=[
            pltpu.VMEM((segs, lines * angles, seg), f32),
            pltpu.VMEM((side * side // seg * lines, seg), f32),
            pltpu.VMEM((2 * side, 2 * side), bf16),
            pltpu.VMEM((angles * segs, seg, seg), bf16),
            pltpu.SemaphoreType.DMA,
        ],
        compiler_params=pltpu.CompilerParams(
            dimension_semantics=("arbitrary",), vmem_limit_bytes=48 * 1024 * 1024
        ),
        name="grid_half",
    )(
        spoke_count, block_index, rows, spoke_angle.reshape(1, spokes), cos_t, sin_t,
        sens_maps[:, 0], kdata[:, :, 0], interp.reshape(angles * segs, seg, seg),
    )

    width = 128
    chunks = side // width
    pp = 4
    npieces = len(coil_rel) // 2
    piece = (2, parts, sub, width)
    kz_total = parts * groups
    order = ((mine_d ^ np.arange(groups, dtype=np.int32))[:, None] * parts + np.arange(parts, dtype=np.int32)[None, :])
    prod = order[:, None, :, None] * order[None, :, None, :] % kz_total
    phase = prod.astype(f32) * (2.0 * jnp.pi / kz_total)
    scale = 1.0 / jnp.sqrt(f32(kz_total))
    cz, sz = jnp.cos(phase) * scale, jnp.sin(phase) * scale
    zmat = jnp.stack([jnp.stack([cz, sz], 3), jnp.stack([-sz, cz], 3)], 1)
    zmat = jnp.transpose(zmat, (0, 1, 3, 2, 4, 5)).reshape(2 * kz_total, 2 * kz_total)

    finals = []
    for j in range(chunks):
        cols = slice(j * width, (j + 1) * width)
        ct, st = cos_h.T[:, cols], sin_h.T[:, cols]
        m2 = np.concatenate([np.concatenate([ct, -st], 1), np.concatenate([st, ct], 1)], 0)
        m2 = jnp.asarray(m2).astype(bf16)
        out_spec = pl.BlockSpec((npieces, 2, pp, sub, width), lambda i: (0, 0, i, 0, 0))
        out_type = jax.ShapeDtypeStruct((npieces,) + piece, f32)
        send, keep = pl.pallas_call(
            image_kernel,
            grid=(parts // pp,),
            in_specs=[
                pl.BlockSpec((pp, side, 2 * side), lambda i: (i, 0, 0)),
                pl.BlockSpec((2 * side, 2 * width), lambda i: (0, 0)),
                pl.BlockSpec((2, side, width), lambda i, j=j: (0, 0, j)),
            ],
            out_specs=[out_spec, out_spec],
            out_shape=[out_type, out_type],
            compiler_params=pltpu.CompilerParams(
                dimension_semantics=("arbitrary",), vmem_limit_bytes=48 * 1024 * 1024
            ),
            name="image_piece",
        )(half, m2, sens_p)
        got = swap(send, "coil", 1)
        q = npieces // 4
        h = q // 2
        x_send = keep[:q] + got[:q]
        y_send = keep[2 * q:3 * q] + got[2 * q:3 * q]
        x_got = swap(x_send, "coil", 2)
        y_got = swap(y_send, "coil", 4)
        x_keep = keep[q:2 * q] + got[q:2 * q]
        y_keep = keep[3 * q:] + got[3 * q:]
        xy_send = x_keep[h:] + x_got[h:]
        yx_send = y_keep[h:] + y_got[h:]
        xy_got = swap(xy_send, "coil", 4)
        yx_got = swap(yx_send, "coil", 2)
        mine = [x_keep[s] + x_got[s] + xy_got[s] for s in range(h)]
        mine += [y_keep[s] + y_got[s] + yx_got[s] for s in range(h)]
        arrived = [mine[0]] + [swap(mine[s], "kz", s) for s in range(1, groups)]
        flat = 2 * parts * sub
        spun = pl.pallas_call(
            kz_kernel,
            out_shape=[jax.ShapeDtypeStruct((flat, width), f32)] * groups,
            name="kz_dft",
        )(zmat, *[v.reshape(flat, width) for v in arrived])
        spun = [v.reshape(piece) for v in spun]
        finals += [spun[0]] + [swap(spun[s], "kz", s) for s in range(1, groups)]
    vm = pl.BlockSpec(memory_space=pltpu.VMEM)
    return pl.pallas_call(
        place_kernel,
        in_specs=[smem] + [vm] * len(finals),
        out_specs=vm,
        out_shape=jax.ShapeDtypeStruct((2, parts, sub * groups, side), f32),
        name="place",
    )(mine_d.reshape(1).astype(jnp.int32), *finals)


def dft_tables(length, dtype):
    index = jnp.arange(length, dtype=jnp.int32)
    product = index[:, None] * index[None, :] % length
    phase = product.astype(jnp.float32) * (2.0 * jnp.pi / length)
    scale = 1.0 / jnp.sqrt(jnp.float32(length))
    return ((jnp.cos(phase) * scale).astype(dtype), (jnp.sin(phase) * scale).astype(dtype))


def kz_block(z_first, z_count, k_count, length):
    z_index = z_first + jnp.arange(z_count, dtype=jnp.int32)
    k_index = jnp.arange(k_count, dtype=jnp.int32)
    product = z_index[:, None] * k_index[None, :] % length
    phase = product.astype(jnp.float32) * (2.0 * jnp.pi / length)
    scale = 1.0 / jnp.sqrt(jnp.float32(length))
    return (jnp.cos(phase) * scale, jnp.sin(phase) * scale)


def kz_apply(cos_z, sin_z, slab):
    high = lax.Precision.HIGHEST
    real_part = jnp.einsum("zk,kyx->zyx", cos_z, slab[0], precision=high) + jnp.einsum(
        "zk,kyx->zyx", sin_z, slab[1], precision=high
    )
    imag_part = jnp.einsum("zk,kyx->zyx", cos_z, slab[1], precision=high) - jnp.einsum(
        "zk,kyx->zyx", sin_z, slab[0], precision=high
    )
    return jnp.stack([real_part, imag_part])


def coil_image(data, weights, interp, block_index, cos_t, sin_t):
    f32 = jnp.float32
    binned = jnp.einsum("rpsn,psa->rpan", data, weights, preferred_element_type=f32).astype(
        jnp.bfloat16
    )
    rdim, pdim, adim, mdim = binned.shape
    seg = interp.shape[2]
    gdim = mdim // seg
    side = cos_t.shape[0]
    pieces = binned.reshape(rdim, pdim, adim, gdim, seg)
    contrib = jnp.einsum("rpagj,agjt->rpagt", pieces, interp, preferred_element_type=f32)
    flat = jnp.zeros((rdim, pdim, side * side // seg, seg), f32)
    flat = flat.at[:, :, block_index.reshape(-1)].add(contrib.reshape(rdim, pdim, adim * gdim, seg))
    grid = flat.reshape(rdim, pdim, side, side).astype(jnp.bfloat16)
    half_re = jnp.einsum("ky,pyx->pkx", cos_t, grid[0], preferred_element_type=f32) + jnp.einsum(
        "ky,pyx->pkx", sin_t, grid[1], preferred_element_type=f32
    )
    half_im = jnp.einsum("ky,pyx->pkx", cos_t, grid[1], preferred_element_type=f32) - jnp.einsum(
        "ky,pyx->pkx", sin_t, grid[0], preferred_element_type=f32
    )
    half_re = half_re.astype(jnp.bfloat16)
    half_im = half_im.astype(jnp.bfloat16)
    out_re = jnp.einsum("pkx,mx->pkm", half_re, cos_t, preferred_element_type=f32) + jnp.einsum(
        "pkx,mx->pkm", half_im, sin_t, preferred_element_type=f32
    )
    out_im = jnp.einsum("pkx,mx->pkm", half_im, cos_t, preferred_element_type=f32) - jnp.einsum(
        "pkx,mx->pkm", half_re, sin_t, preferred_element_type=f32
    )
    return jnp.stack([out_re, out_im])


def conj_product(sens, image):
    real_part = sens[0] * image[0] + sens[1] * image[1]
    imag_part = sens[0] * image[1] - sens[1] * image[0]
    return jnp.stack([real_part, imag_part])


def per_device(kdata, spoke_angle, spoke_count, block_index, interp, sens_maps):
    side = sens_maps.shape[2]
    parts_here = kdata.shape[1]
    spokes = kdata.shape[3]
    angles = interp.shape[0]
    cos_t, sin_t = dft_tables(side, jnp.bfloat16)
    position = jnp.arange(spokes, dtype=jnp.int32)
    used = position[None, :] < spoke_count[:, None]
    match = spoke_angle[:, None] == jnp.arange(angles, dtype=jnp.int32)[None, :]
    weights = (used[:, :, None] & match[None, :, :]).astype(jnp.bfloat16)
    data = kdata[:, :, 0]
    image_c = coil_image(data, weights, interp, block_index, cos_t, sin_t)
    sens_here = sens_maps.astype(jnp.float32)
    weighted = conj_product(sens_here[:, 0][:, None], image_c)
    combined = lax.psum_scatter(weighted, "coil", scatter_dimension=2, tiled=True)
    groups = lax.axis_size("kz")
    kz_total = parts_here * groups
    my_first = lax.axis_index("kz") * parts_here
    piece = lax.all_gather(combined, "kz", axis=1, tiled=True)
    cos_z, sin_z = kz_block(my_first, parts_here, piece.shape[1], kz_total)
    return kz_apply(cos_z, sin_z, piece)


def solution(mesh):
    placed = (
        P(None, "kz", "coil", None, None),
        P(),
        P("kz"),
        P(),
        P(),
        P(None, "coil", None, None),
    )
    fast = mesh.shape["coil"] == 8 and mesh.shape["kz"] == 4
    return jax.shard_map(
        fast_device if fast else per_device,
        mesh=mesh,
        in_specs=placed,
        out_specs=P(None, "kz", "coil", None),
        check_vma=False,
    )
```

```python
import functools

import jax
import jax.numpy as jnp
import numpy as np
from jax import lax
from jax.experimental import pallas as pl
from jax.experimental.pallas import tpu as pltpu
from jax.sharding import PartitionSpec as P

ROW_CUTS = 2


def host_tables(length, dtype):
    index = np.arange(length, dtype=np.int32)
    product = index[:, None] * index[None, :] % length
    phase = product.astype(np.float32) * np.float32(2.0 * np.pi / length)
    scale = np.float32(1.0) / np.sqrt(np.float32(length))
    return ((np.cos(phase) * scale).astype(dtype), (np.sin(phase) * scale).astype(dtype))


def grid_kernel(
    count_ref, bidx_ref, rows_ref, angle_ref, table_ref, sens_ref, data_ref, interp_hbm,
    half_ref, sensp_ref,
    bin_ref, grid_ref, m1_ref, interp_ref, sem,
):
    f32, bf16 = jnp.float32, jnp.bfloat16
    step = pl.program_id(0)
    parts = pl.num_programs(0) // 2
    angles, segs = bidx_ref.shape
    seg = interp_ref.shape[1]
    side = table_ref.shape[0]
    spokes = angle_ref.shape[1]
    lines = 2 * bin_ref.shape[1] // (2 * angles)
    nblocks = grid_ref.shape[0] // lines
    per_row = side // seg
    nparts = lines // 2

    @pl.when(step == 0)
    def _():
        pltpu.make_async_copy(interp_hbm, interp_ref, sem).start()
        pick = (lax.broadcasted_iota(jnp.int32, (side, side), 1) == rows_ref[...]).astype(bf16)
        both = jnp.dot(pick, table_ref[...], preferred_element_type=f32)
        pc, ps = both[:, :side], both[:, side:]
        m1_ref[:side, :side] = pc.astype(bf16)
        m1_ref[:side, side:] = ps.astype(bf16)
        m1_ref[side:, :side] = (-ps).astype(bf16)
        m1_ref[side:, side:] = pc.astype(bf16)
        for r in range(2):
            sensp_ref[r] = jnp.dot(pick, sens_ref[r], preferred_element_type=f32)

    @pl.when(step < parts)
    def _():
        zrows = grid_ref.shape[0] // nparts
        grid_ref[pl.ds(step * zrows, zrows), :] = jnp.zeros((zrows, seg), f32)
        a_iota = lax.broadcasted_iota(jnp.int32, (angles, spokes), 0)
        s_iota = lax.broadcasted_iota(jnp.int32, (angles, spokes), 1)
        keep = (a_iota == angle_ref[...]) & (s_iota < count_ref[step])
        wt = jnp.where(keep, 1.0, 0.0).astype(bf16)
        for r in range(2):
            b = jnp.dot(wt, data_ref[r, 0], preferred_element_type=f32)
            b = b.astype(bf16).astype(f32)
            for g in range(segs):
                bin_ref[g, pl.ds((r * nparts + step) * angles, angles), :] = b[:, g * seg:(g + 1) * seg]

    @pl.when(step == parts)
    def _():
        pltpu.make_async_copy(interp_hbm, interp_ref, sem).wait()
        unroll = 4 if angles % 4 == 0 else 1

        def body(i, carry):
            res = []
            for u in range(unroll):
                a = i * unroll + u
                for g in range(0, segs, 2):
                    lhs = jnp.concatenate(
                        [bin_ref[g + k, pl.ds(a, lines, stride=angles), :].astype(bf16) for k in range(2)], axis=0
                    )
                    rhs = jnp.concatenate([interp_ref[a * segs + g + k] for k in range(2)], axis=1)
                    both = jnp.dot(lhs, rhs, preferred_element_type=f32)
                    for k in range(2):
                        res.append((bidx_ref[a, g + k], both[k * lines:(k + 1) * lines, k * seg:(k + 1) * seg]))
            for b, v in res:
                at = pl.ds(pl.multiple_of(b * lines, lines), lines)
                grid_ref[at, :] = grid_ref[at, :] + v
            return carry

        lax.fori_loop(0, angles // unroll, body, 0)

    @pl.when(step >= parts)
    def _():
        p = step - parts
        stacked = jnp.concatenate(
            [
                jnp.concatenate(
                    [
                        grid_ref[pl.ds(h * lines + r * nparts + p, side, stride=per_row * lines), :].astype(bf16)
                        for h in range(per_row)
                    ],
                    axis=1,
                )
                for r in range(2)
            ],
            axis=0,
        )
        half = jnp.dot(m1_ref[...], stacked, preferred_element_type=f32).astype(bf16)
        half_ref[0, :, :side] = half[:side]
        half_ref[0, :, side:] = half[side:]


def image_kernel(half_ref, m2_ref, sens_ref, send_ref, keep_ref):
    pp, nrows, depth = half_ref.shape
    width = m2_ref.shape[1] // 2
    pieces = keep_ref.shape[0]
    sub = nrows // (2 * pieces)
    out = jnp.dot(half_ref[...].reshape(pp * nrows, depth), m2_ref[...], preferred_element_type=jnp.float32)
    for q in range(pp):
        re = out[q * nrows:(q + 1) * nrows, :width]
        im = out[q * nrows:(q + 1) * nrows, width:]
        w = (sens_ref[0] * re + sens_ref[1] * im, sens_ref[0] * im - sens_ref[1] * re)
        for r in range(2):
            for m in range(pieces):
                keep_ref[m, r, q * sub:(q + 1) * sub, :] = w[r][m * sub:(m + 1) * sub]
                send_ref[m, r, q * sub:(q + 1) * sub, :] = w[r][(pieces + m) * sub:(pieces + m + 1) * sub]


def kz_kernel(cnt, z_ref, *refs):
    n = len(refs) // 2
    ins, outs = refs[:n], refs[n:]
    rows, width = ins[0].shape
    sub = rows // (2 * cnt)
    x = jnp.concatenate(
        [
            jnp.concatenate(
                [ins[s][pl.ds(r * cnt * sub + i, cnt, stride=sub), :] for s in range(n) for r in range(2)], axis=0
            )
            for i in range(sub)
        ],
        axis=1,
    )
    y = jnp.dot(z_ref[...], x, preferred_element_type=jnp.float32, precision=lax.Precision.HIGHEST)
    for s in range(n):
        for r in range(2):
            for i in range(sub):
                outs[s][pl.ds(r * cnt * sub + i, cnt, stride=sub), :] = y[
                    (s * 2 + r) * cnt:(s * 2 + r + 1) * cnt, i * width:(i + 1) * width
                ]


def place_kernel(me_ref, *refs):
    out_ref = refs[-1]
    ins = refs[:-1]
    _, cnt, _, side = out_ref.shape
    width = ins[0].shape[1]
    sub = ins[0].shape[0] // (2 * cnt)
    cuts = side // width
    n = len(ins) // (cuts * ROW_CUTS)
    for j in range(cuts):
        for s in range(n):
            at = pl.multiple_of((me_ref[0] ^ s) * (sub * ROW_CUTS), sub * ROW_CUTS)
            for r in range(2):
                for z in range(cnt):
                    k = (r * cnt + z) * sub
                    out_ref[r, z, pl.ds(at, sub * ROW_CUTS), j * width:(j + 1) * width] = jnp.concatenate(
                        [ins[(t * cuts + j) * n + s][k:k + sub, :] for t in range(ROW_CUTS)], axis=0
                    )


def swap(x, axis, bit):
    n = lax.axis_size(axis)
    return lax.ppermute(x, axis, [(i, i ^ bit) for i in range(n)])


def piece_order():
    order = []
    for relc in range(2):
        order += [(relc, 1, ry, rd) for ry in range(2) for rd in (0, 1)]
        order += [(relc, 0, ry, rd) for ry in range(2) for rd in (0, 1)]
        order += [(relc, rx, 1, rd) for rx in range(2) for rd in (2, 3)]
        order += [(relc, rx, 0, rd) for rx in range(2) for rd in (2, 3)]
    coil_rel = np.array([c + 2 * x + 4 * y for c, x, y, d in order], np.int32)
    kz_rel = np.array([d for c, x, y, d in order], np.int32)
    return coil_rel, kz_rel


def fast_device(kdata, spoke_angle, spoke_count, block_index, interp, sens_maps):
    f32, bf16 = jnp.float32, jnp.bfloat16
    _, parts, _, spokes, samples = kdata.shape
    side = sens_maps.shape[2]
    angles, segs, seg, _ = interp.shape
    groups = lax.axis_size("kz")
    mine_c = lax.axis_index("coil")
    mine_d = lax.axis_index("kz")
    full = side // (lax.axis_size("coil") * groups)
    sub = full // ROW_CUTS
    coil_rel, kz_rel = piece_order()
    starts = (mine_c ^ coil_rel) * (full * groups) + (mine_d ^ kz_rel) * full
    offset = np.arange(ROW_CUTS * sub, dtype=np.int32).reshape(ROW_CUTS, 1, sub)
    rows = (starts[None, :, None] + offset).reshape(side, 1)
    cos_h, sin_h = host_tables(side, np.float32)
    table = jnp.asarray(np.concatenate([cos_h, sin_h], 1).astype(bf16))
    lines = 2 * parts
    smem = pl.BlockSpec(memory_space=pltpu.SMEM)
    whole = lambda shape: pl.BlockSpec(shape, lambda i: (0,) * len(shape))
    half, sens_p = pl.pallas_call(
        grid_kernel,
        grid=(2 * parts,),
        in_specs=[
            smem, smem, whole((side, 1)), whole((1, spokes)), whole((side, 2 * side)),
            whole((2, side, side)),
            pl.BlockSpec((2, 1, spokes, samples), lambda i: (0, jnp.minimum(i, parts - 1), 0, 0)),
            pl.BlockSpec(memory_space=pl.ANY),
        ],
        out_specs=[
            pl.BlockSpec((1, side, 2 * side), lambda i: (jnp.maximum(i - parts, 0), 0, 0)),
            whole((2, side, side)),
        ],
        out_shape=[
            jax.ShapeDtypeStruct((parts, side, 2 * side), bf16),
            jax.ShapeDtypeStruct((2, side, side), f32),
        ],
        scratch_shapes=[
            pltpu.VMEM((segs, lines * angles, seg), f32),
            pltpu.VMEM((side * side // seg * lines, seg), f32),
            pltpu.VMEM((2 * side, 2 * side), bf16),
            pltpu.VMEM((angles * segs, seg, seg), bf16),
            pltpu.SemaphoreType.DMA,
        ],
        compiler_params=pltpu.CompilerParams(
            dimension_semantics=("arbitrary",), vmem_limit_bytes=48 * 1024 * 1024
        ),
        name="grid_half",
    )(
        spoke_count, block_index, rows, spoke_angle.reshape(1, spokes), table,
        sens_maps[:, 0], kdata[:, :, 0], interp.reshape(angles * segs, seg, seg),
    )

    width = 128
    chunks = side // width
    pp = 4
    npieces = len(coil_rel) // 2
    flat = 2 * parts * sub
    nrows = side // ROW_CUTS
    kz_total = parts * groups
    order = ((mine_d ^ np.arange(groups, dtype=np.int32))[:, None] * parts + np.arange(parts, dtype=np.int32)[None, :])
    prod = order[:, None, :, None] * order[None, :, None, :] % kz_total
    phase = prod.astype(f32) * (2.0 * jnp.pi / kz_total)
    scale = 1.0 / jnp.sqrt(f32(kz_total))
    cz, sz = jnp.cos(phase) * scale, jnp.sin(phase) * scale
    zmat = jnp.stack([jnp.stack([cz, sz], 3), jnp.stack([-sz, cz], 3)], 1)
    zmat = jnp.transpose(zmat, (0, 1, 3, 2, 4, 5)).reshape(2 * kz_total, 2 * kz_total)

    finals = []
    for t, j in [(t, j) for t in range(ROW_CUTS) for j in range(chunks)]:
        cols = slice(j * width, (j + 1) * width)
        ct, st = cos_h.T[:, cols], sin_h.T[:, cols]
        m2 = np.concatenate([np.concatenate([ct, -st], 1), np.concatenate([st, ct], 1)], 0)
        m2 = jnp.asarray(m2.astype(bf16))
        out_spec = pl.BlockSpec((npieces, 2, pp * sub, width), lambda i: (0, 0, i, 0))
        out_type = jax.ShapeDtypeStruct((npieces, 2, parts * sub, width), f32)
        send, keep = pl.pallas_call(
            image_kernel,
            grid=(parts // pp,),
            in_specs=[
                pl.BlockSpec((pp, nrows, 2 * side), lambda i, t=t: (i, t, 0)),
                pl.BlockSpec((2 * side, 2 * width), lambda i: (0, 0)),
                pl.BlockSpec((2, nrows, width), lambda i, t=t, j=j: (0, t, j)),
            ],
            out_specs=[out_spec, out_spec],
            out_shape=[out_type, out_type],
            compiler_params=pltpu.CompilerParams(
                dimension_semantics=("arbitrary",), vmem_limit_bytes=48 * 1024 * 1024
            ),
            name="image_piece",
        )(half, m2, sens_p)
        got = swap(send, "coil", 1)
        q = npieces // 4
        h = q // 2
        x_send = keep[:q] + got[:q]
        y_send = keep[2 * q:3 * q] + got[2 * q:3 * q]
        x_got = swap(x_send, "coil", 2)
        y_got = swap(y_send, "coil", 4)
        x_keep = keep[q:2 * q] + got[q:2 * q]
        y_keep = keep[3 * q:] + got[3 * q:]
        xy_send = x_keep[h:] + x_got[h:]
        yx_send = y_keep[h:] + y_got[h:]
        xy_got = swap(xy_send, "coil", 4)
        yx_got = swap(yx_send, "coil", 2)
        mine = [x_keep[s] + x_got[s] + xy_got[s] for s in range(h)]
        mine += [y_keep[s] + y_got[s] + yx_got[s] for s in range(h)]
        arrived = [mine[0]] + [swap(mine[s], "kz", s) for s in range(1, groups)]
        spun = pl.pallas_call(
            functools.partial(kz_kernel, parts),
            out_shape=[jax.ShapeDtypeStruct((flat, width), f32)] * groups,
            name="kz_dft",
        )(zmat, *[v.reshape(flat, width) for v in arrived])
        finals += [spun[0]] + [swap(spun[s], "kz", s) for s in range(1, groups)]
    vm = pl.BlockSpec(memory_space=pltpu.VMEM)
    return pl.pallas_call(
        place_kernel,
        in_specs=[smem] + [vm] * len(finals),
        out_specs=vm,
        out_shape=jax.ShapeDtypeStruct((2, parts, full * groups, side), f32),
        name="place",
    )(mine_d.reshape(1).astype(jnp.int32), *finals)


def dft_tables(length, dtype):
    index = jnp.arange(length, dtype=jnp.int32)
    product = index[:, None] * index[None, :] % length
    phase = product.astype(jnp.float32) * (2.0 * jnp.pi / length)
    scale = 1.0 / jnp.sqrt(jnp.float32(length))
    return ((jnp.cos(phase) * scale).astype(dtype), (jnp.sin(phase) * scale).astype(dtype))


def kz_block(z_first, z_count, k_count, length):
    z_index = z_first + jnp.arange(z_count, dtype=jnp.int32)
    k_index = jnp.arange(k_count, dtype=jnp.int32)
    product = z_index[:, None] * k_index[None, :] % length
    phase = product.astype(jnp.float32) * (2.0 * jnp.pi / length)
    scale = 1.0 / jnp.sqrt(jnp.float32(length))
    return (jnp.cos(phase) * scale, jnp.sin(phase) * scale)


def kz_apply(cos_z, sin_z, slab):
    high = lax.Precision.HIGHEST
    real_part = jnp.einsum("zk,kyx->zyx", cos_z, slab[0], precision=high) + jnp.einsum(
        "zk,kyx->zyx", sin_z, slab[1], precision=high
    )
    imag_part = jnp.einsum("zk,kyx->zyx", cos_z, slab[1], precision=high) - jnp.einsum(
        "zk,kyx->zyx", sin_z, slab[0], precision=high
    )
    return jnp.stack([real_part, imag_part])


def coil_image(data, weights, interp, block_index, cos_t, sin_t):
    f32 = jnp.float32
    binned = jnp.einsum("rpsn,psa->rpan", data, weights, preferred_element_type=f32).astype(
        jnp.bfloat16
    )
    rdim, pdim, adim, mdim = binned.shape
    seg = interp.shape[2]
    gdim = mdim // seg
    side = cos_t.shape[0]
    pieces = binned.reshape(rdim, pdim, adim, gdim, seg)
    contrib = jnp.einsum("rpagj,agjt->rpagt", pieces, interp, preferred_element_type=f32)
    flat = jnp.zeros((rdim, pdim, side * side // seg, seg), f32)
    flat = flat.at[:, :, block_index.reshape(-1)].add(contrib.reshape(rdim, pdim, adim * gdim, seg))
    grid = flat.reshape(rdim, pdim, side, side).astype(jnp.bfloat16)
    half_re = jnp.einsum("ky,pyx->pkx", cos_t, grid[0], preferred_element_type=f32) + jnp.einsum(
        "ky,pyx->pkx", sin_t, grid[1], preferred_element_type=f32
    )
    half_im = jnp.einsum("ky,pyx->pkx", cos_t, grid[1], preferred_element_type=f32) - jnp.einsum(
        "ky,pyx->pkx", sin_t, grid[0], preferred_element_type=f32
    )
    half_re = half_re.astype(jnp.bfloat16)
    half_im = half_im.astype(jnp.bfloat16)
    out_re = jnp.einsum("pkx,mx->pkm", half_re, cos_t, preferred_element_type=f32) + jnp.einsum(
        "pkx,mx->pkm", half_im, sin_t, preferred_element_type=f32
    )
    out_im = jnp.einsum("pkx,mx->pkm", half_im, cos_t, preferred_element_type=f32) - jnp.einsum(
        "pkx,mx->pkm", half_re, sin_t, preferred_element_type=f32
    )
    return jnp.stack([out_re, out_im])


def conj_product(sens, image):
    real_part = sens[0] * image[0] + sens[1] * image[1]
    imag_part = sens[0] * image[1] - sens[1] * image[0]
    return jnp.stack([real_part, imag_part])


def per_device(kdata, spoke_angle, spoke_count, block_index, interp, sens_maps):
    side = sens_maps.shape[2]
    parts_here = kdata.shape[1]
    spokes = kdata.shape[3]
    angles = interp.shape[0]
    cos_t, sin_t = dft_tables(side, jnp.bfloat16)
    position = jnp.arange(spokes, dtype=jnp.int32)
    used = position[None, :] < spoke_count[:, None]
    match = spoke_angle[:, None] == jnp.arange(angles, dtype=jnp.int32)[None, :]
    weights = (used[:, :, None] & match[None, :, :]).astype(jnp.bfloat16)
    data = kdata[:, :, 0]
    image_c = coil_image(data, weights, interp, block_index, cos_t, sin_t)
    sens_here = sens_maps.astype(jnp.float32)
    weighted = conj_product(sens_here[:, 0][:, None], image_c)
    combined = lax.psum_scatter(weighted, "coil", scatter_dimension=2, tiled=True)
    groups = lax.axis_size("kz")
    kz_total = parts_here * groups
    my_first = lax.axis_index("kz") * parts_here
    piece = lax.all_gather(combined, "kz", axis=1, tiled=True)
    cos_z, sin_z = kz_block(my_first, parts_here, piece.shape[1], kz_total)
    return kz_apply(cos_z, sin_z, piece)


def solution(mesh):
    placed = (
        P(None, "kz", "coil", None, None),
        P(),
        P("kz"),
        P(),
        P(),
        P(None, "coil", None, None),
    )
    fast = mesh.shape["coil"] == 8 and mesh.shape["kz"] == 4
    return jax.shard_map(
        fast_device if fast else per_device,
        mesh=mesh,
        in_specs=placed,
        out_specs=P(None, "kz", "coil", None),
        check_vma=False,
    )
```

```python
import functools

import jax
import jax.numpy as jnp
import numpy as np
from jax import lax
from jax.experimental import pallas as pl
from jax.experimental.pallas import tpu as pltpu
from jax.sharding import PartitionSpec as P

ROW_CUTS = 1


def host_tables(length, dtype):
    index = np.arange(length, dtype=np.int32)
    product = index[:, None] * index[None, :] % length
    phase = product.astype(np.float32) * np.float32(2.0 * np.pi / length)
    scale = np.float32(1.0) / np.sqrt(np.float32(length))
    return ((np.cos(phase) * scale).astype(dtype), (np.sin(phase) * scale).astype(dtype))


def grid_kernel(
    count_ref, bidx_ref, rows_ref, angle_ref, table_ref, sens_ref, data_ref, interp_hbm,
    half_ref, sensp_ref,
    bin_ref, grid_ref, m1_ref, interp_ref, sem,
):
    f32, bf16 = jnp.float32, jnp.bfloat16
    step = pl.program_id(0)
    group = data_ref.shape[1]
    parts = pl.num_programs(0) // 2
    angles, segs = bidx_ref.shape
    seg = interp_ref.shape[1]
    side = table_ref.shape[0]
    spokes = angle_ref.shape[1]
    lines = 2 * bin_ref.shape[1] // (2 * angles)
    nblocks = grid_ref.shape[0] // lines
    per_row = side // seg
    nparts = lines // 2

    @pl.when(step == 0)
    def _():
        pltpu.make_async_copy(interp_hbm, interp_ref, sem).start()
        pick = (lax.broadcasted_iota(jnp.int32, (side, side), 1) == rows_ref[...]).astype(bf16)
        both = jnp.dot(pick, table_ref[...], preferred_element_type=f32)
        pc, ps = both[:, :side], both[:, side:]
        m1_ref[:side, :side] = pc.astype(bf16)
        m1_ref[:side, side:] = ps.astype(bf16)
        m1_ref[side:, :side] = (-ps).astype(bf16)
        m1_ref[side:, side:] = pc.astype(bf16)
        for r in range(2):
            sensp_ref[r] = jnp.dot(pick, sens_ref[r], preferred_element_type=f32)

    @pl.when(step < parts)
    def _():
        zrows = grid_ref.shape[0] // parts
        grid_ref[pl.ds(step * zrows, zrows), :] = jnp.zeros((zrows, seg), f32)
        a_iota = lax.broadcasted_iota(jnp.int32, (angles, spokes), 0)
        s_iota = lax.broadcasted_iota(jnp.int32, (angles, spokes), 1)
        for q in range(group):
            part = step * group + q
            keep = (a_iota == angle_ref[...]) & (s_iota < count_ref[part])
            wt = jnp.where(keep, 1.0, 0.0).astype(bf16)
            for r in range(2):
                b = jnp.dot(wt, data_ref[r, q], preferred_element_type=f32)
                b = b.astype(bf16).astype(f32)
                for g in range(segs):
                    bin_ref[g, pl.ds((r * nparts + part) * angles, angles), :] = b[:, g * seg:(g + 1) * seg]

    @pl.when(step == parts)
    def _():
        pltpu.make_async_copy(interp_hbm, interp_ref, sem).wait()
        unroll = 4 if angles % 4 == 0 else 1

        def body(i, carry):
            res = []
            for u in range(unroll):
                a = i * unroll + u
                for g in range(0, segs, 2):
                    lhs = jnp.concatenate(
                        [bin_ref[g + k, pl.ds(a, lines, stride=angles), :].astype(bf16) for k in range(2)], axis=0
                    )
                    rhs = jnp.concatenate([interp_ref[a * segs + g + k] for k in range(2)], axis=1)
                    both = jnp.dot(lhs, rhs, preferred_element_type=f32)
                    for k in range(2):
                        res.append((bidx_ref[a, g + k], both[k * lines:(k + 1) * lines, k * seg:(k + 1) * seg]))
            for b, v in res:
                at = pl.ds(pl.multiple_of(b * lines, lines), lines)
                grid_ref[at, :] = grid_ref[at, :] + v
            return carry

        lax.fori_loop(0, angles // unroll, body, 0)

    @pl.when(step >= parts)
    def _():
        for q in range(group):
            p = (step - parts) * group + q
            stacked = jnp.concatenate(
                [
                    jnp.concatenate(
                        [
                            grid_ref[pl.ds(h * lines + r * nparts + p, side, stride=per_row * lines), :].astype(bf16)
                            for h in range(per_row)
                        ],
                        axis=1,
                    )
                    for r in range(2)
                ],
                axis=0,
            )
            half = jnp.dot(m1_ref[...], stacked, preferred_element_type=f32).astype(bf16)
            half_ref[q, :, :side] = half[:side]
            half_ref[q, :, side:] = half[side:]


def image_kernel(half_ref, m2_ref, sens_ref, send_ref, keep_ref):
    pp, nrows, depth = half_ref.shape
    width = m2_ref.shape[1] // 2
    pieces = keep_ref.shape[0]
    sub = nrows // (2 * pieces)
    out = jnp.dot(half_ref[...].reshape(pp * nrows, depth), m2_ref[...], preferred_element_type=jnp.float32)
    for q in range(pp):
        re = out[q * nrows:(q + 1) * nrows, :width]
        im = out[q * nrows:(q + 1) * nrows, width:]
        w = (sens_ref[0] * re + sens_ref[1] * im, sens_ref[0] * im - sens_ref[1] * re)
        for r in range(2):
            for m in range(pieces):
                keep_ref[m, r, q * sub:(q + 1) * sub, :] = w[r][m * sub:(m + 1) * sub]
                send_ref[m, r, q * sub:(q + 1) * sub, :] = w[r][(pieces + m) * sub:(pieces + m + 1) * sub]


def kz_kernel(cnt, z_ref, *refs):
    n = len(refs) // 2
    ins, outs = refs[:n], refs[n:]
    rows, width = ins[0].shape
    sub = rows // (2 * cnt)
    x = jnp.concatenate(
        [
            jnp.concatenate(
                [ins[s][pl.ds(r * cnt * sub + i, cnt, stride=sub), :] for s in range(n) for r in range(2)], axis=0
            )
            for i in range(sub)
        ],
        axis=1,
    )
    y = jnp.dot(z_ref[...], x, preferred_element_type=jnp.float32, precision=lax.Precision.HIGHEST)
    for s in range(n):
        for r in range(2):
            for i in range(sub):
                outs[s][pl.ds(r * cnt * sub + i, cnt, stride=sub), :] = y[
                    (s * 2 + r) * cnt:(s * 2 + r + 1) * cnt, i * width:(i + 1) * width
                ]


def place_kernel(me_ref, *refs):
    out_ref = refs[-1]
    ins = refs[:-1]
    _, cnt, _, side = out_ref.shape
    width = ins[0].shape[1]
    sub = ins[0].shape[0] // (2 * cnt)
    cuts = side // width
    n = len(ins) // (cuts * ROW_CUTS)
    for j in range(cuts):
        for s in range(n):
            at = pl.multiple_of((me_ref[0] ^ s) * (sub * ROW_CUTS), sub * ROW_CUTS)
            for r in range(2):
                for z in range(cnt):
                    k = (r * cnt + z) * sub
                    out_ref[r, z, pl.ds(at, sub * ROW_CUTS), j * width:(j + 1) * width] = jnp.concatenate(
                        [ins[(t * cuts + j) * n + s][k:k + sub, :] for t in range(ROW_CUTS)], axis=0
                    )


def swap(x, axis, bit):
    n = lax.axis_size(axis)
    return lax.ppermute(x, axis, [(i, i ^ bit) for i in range(n)])


def piece_order():
    order = []
    for relc in range(2):
        order += [(relc, 1, ry, rd) for ry in range(2) for rd in (0, 1)]
        order += [(relc, 0, ry, rd) for ry in range(2) for rd in (0, 1)]
        order += [(relc, rx, 1, rd) for rx in range(2) for rd in (2, 3)]
        order += [(relc, rx, 0, rd) for rx in range(2) for rd in (2, 3)]
    coil_rel = np.array([c + 2 * x + 4 * y for c, x, y, d in order], np.int32)
    kz_rel = np.array([d for c, x, y, d in order], np.int32)
    return coil_rel, kz_rel


def fast_device(kdata, spoke_angle, spoke_count, block_index, interp, sens_maps):
    f32, bf16 = jnp.float32, jnp.bfloat16
    _, parts, _, spokes, samples = kdata.shape
    side = sens_maps.shape[2]
    angles, segs, seg, _ = interp.shape
    groups = lax.axis_size("kz")
    mine_c = lax.axis_index("coil")
    mine_d = lax.axis_index("kz")
    full = side // (lax.axis_size("coil") * groups)
    sub = full // ROW_CUTS
    coil_rel, kz_rel = piece_order()
    starts = (mine_c ^ coil_rel) * (full * groups) + (mine_d ^ kz_rel) * full
    offset = np.arange(ROW_CUTS * sub, dtype=np.int32).reshape(ROW_CUTS, 1, sub)
    rows = (starts[None, :, None] + offset).reshape(side, 1)
    cos_h, sin_h = host_tables(side, np.float32)
    table = jnp.asarray(np.concatenate([cos_h, sin_h], 1).astype(bf16))
    lines = 2 * parts
    pp = 8
    steps = parts // pp
    smem = pl.BlockSpec(memory_space=pltpu.SMEM)
    whole = lambda shape: pl.BlockSpec(shape, lambda i: (0,) * len(shape))
    half, sens_p = pl.pallas_call(
        grid_kernel,
        grid=(2 * steps,),
        in_specs=[
            smem, smem, whole((side, 1)), whole((1, spokes)), whole((side, 2 * side)),
            whole((2, side, side)),
            pl.BlockSpec((2, pp, spokes, samples), lambda i: (0, jnp.minimum(i, steps - 1), 0, 0)),
            pl.BlockSpec(memory_space=pl.ANY),
        ],
        out_specs=[
            pl.BlockSpec((pp, side, 2 * side), lambda i: (jnp.maximum(i - steps, 0), 0, 0)),
            whole((2, side, side)),
        ],
        out_shape=[
            jax.ShapeDtypeStruct((parts, side, 2 * side), bf16),
            jax.ShapeDtypeStruct((2, side, side), f32),
        ],
        scratch_shapes=[
            pltpu.VMEM((segs, lines * angles, seg), f32),
            pltpu.VMEM((side * side // seg * lines, seg), f32),
            pltpu.VMEM((2 * side, 2 * side), bf16),
            pltpu.VMEM((angles * segs, seg, seg), bf16),
            pltpu.SemaphoreType.DMA,
        ],
        compiler_params=pltpu.CompilerParams(
            dimension_semantics=("arbitrary",), vmem_limit_bytes=48 * 1024 * 1024
        ),
        name="grid_half",
    )(
        spoke_count, block_index, rows, spoke_angle.reshape(1, spokes), table,
        sens_maps[:, 0], kdata[:, :, 0], interp.reshape(angles * segs, seg, seg),
    )

    width = 128
    chunks = side // width
    npieces = len(coil_rel) // 2
    flat = 2 * parts * sub
    nrows = side // ROW_CUTS
    kz_total = parts * groups
    order = ((mine_d ^ np.arange(groups, dtype=np.int32))[:, None] * parts + np.arange(parts, dtype=np.int32)[None, :])
    prod = order[:, None, :, None] * order[None, :, None, :] % kz_total
    phase = prod.astype(f32) * (2.0 * jnp.pi / kz_total)
    scale = 1.0 / jnp.sqrt(f32(kz_total))
    cz, sz = jnp.cos(phase) * scale, jnp.sin(phase) * scale
    zmat = jnp.stack([jnp.stack([cz, sz], 3), jnp.stack([-sz, cz], 3)], 1)
    zmat = jnp.transpose(zmat, (0, 1, 3, 2, 4, 5)).reshape(2 * kz_total, 2 * kz_total)

    finals = []
    before = None
    for t, j in [(t, j) for t in range(ROW_CUTS) for j in range(chunks)]:
        cols = slice(j * width, (j + 1) * width)
        ct, st = cos_h.T[:, cols], sin_h.T[:, cols]
        m2 = np.concatenate([np.concatenate([ct, -st], 1), np.concatenate([st, ct], 1)], 0)
        m2 = jnp.asarray(m2.astype(bf16))
        out_spec = pl.BlockSpec((npieces, 2, pp * sub, width), lambda i: (0, 0, i, 0))
        out_type = jax.ShapeDtypeStruct((npieces, 2, parts * sub, width), f32)
        send, keep = pl.pallas_call(
            image_kernel,
            grid=(parts // pp,),
            in_specs=[
                pl.BlockSpec((pp, nrows, 2 * side), lambda i, t=t: (i, t, 0)),
                pl.BlockSpec((2 * side, 2 * width), lambda i: (0, 0)),
                pl.BlockSpec((2, nrows, width), lambda i, t=t, j=j: (0, t, j)),
            ],
            out_specs=[out_spec, out_spec],
            out_shape=[out_type, out_type],
            compiler_params=pltpu.CompilerParams(
                dimension_semantics=("arbitrary",), vmem_limit_bytes=48 * 1024 * 1024
            ),
            name="image_piece",
        )(half, m2, sens_p)
        got = swap(send, "coil", 1)
        q = npieces // 4
        h = q // 2
        if before is not None:
            got, *before = lax.optimization_barrier((got, *before))
        x_send = keep[:q] + got[:q]
        y_send = keep[2 * q:3 * q] + got[2 * q:3 * q]
        x_got = swap(x_send, "coil", 2)
        y_got = swap(y_send, "coil", 4)
        x_keep = keep[q:2 * q] + got[q:2 * q]
        y_keep = keep[3 * q:] + got[3 * q:]
        xy_send = x_keep[h:] + x_got[h:]
        yx_send = y_keep[h:] + y_got[h:]
        before = (xy_send, yx_send)
        xy_got = swap(xy_send, "coil", 4)
        yx_got = swap(yx_send, "coil", 2)
        mine = [x_keep[s] + x_got[s] + xy_got[s] for s in range(h)]
        mine += [y_keep[s] + y_got[s] + yx_got[s] for s in range(h)]
        arrived = [mine[0]] + [swap(mine[s], "kz", s) for s in range(1, groups)]
        spun = pl.pallas_call(
            functools.partial(kz_kernel, parts),
            out_shape=[jax.ShapeDtypeStruct((flat, width), f32)] * groups,
            name="kz_dft",
        )(zmat, *[v.reshape(flat, width) for v in arrived])
        finals += [spun[0]] + [swap(spun[s], "kz", s) for s in range(1, groups)]
    vm = pl.BlockSpec(memory_space=pltpu.VMEM)
    return pl.pallas_call(
        place_kernel,
        in_specs=[smem] + [vm] * len(finals),
        out_specs=vm,
        out_shape=jax.ShapeDtypeStruct((2, parts, full * groups, side), f32),
        name="place",
    )(mine_d.reshape(1).astype(jnp.int32), *finals)


def dft_tables(length, dtype):
    index = jnp.arange(length, dtype=jnp.int32)
    product = index[:, None] * index[None, :] % length
    phase = product.astype(jnp.float32) * (2.0 * jnp.pi / length)
    scale = 1.0 / jnp.sqrt(jnp.float32(length))
    return ((jnp.cos(phase) * scale).astype(dtype), (jnp.sin(phase) * scale).astype(dtype))


def kz_block(z_first, z_count, k_count, length):
    z_index = z_first + jnp.arange(z_count, dtype=jnp.int32)
    k_index = jnp.arange(k_count, dtype=jnp.int32)
    product = z_index[:, None] * k_index[None, :] % length
    phase = product.astype(jnp.float32) * (2.0 * jnp.pi / length)
    scale = 1.0 / jnp.sqrt(jnp.float32(length))
    return (jnp.cos(phase) * scale, jnp.sin(phase) * scale)


def kz_apply(cos_z, sin_z, slab):
    high = lax.Precision.HIGHEST
    real_part = jnp.einsum("zk,kyx->zyx", cos_z, slab[0], precision=high) + jnp.einsum(
        "zk,kyx->zyx", sin_z, slab[1], precision=high
    )
    imag_part = jnp.einsum("zk,kyx->zyx", cos_z, slab[1], precision=high) - jnp.einsum(
        "zk,kyx->zyx", sin_z, slab[0], precision=high
    )
    return jnp.stack([real_part, imag_part])


def coil_image(data, weights, interp, block_index, cos_t, sin_t):
    f32 = jnp.float32
    binned = jnp.einsum("rpsn,psa->rpan", data, weights, preferred_element_type=f32).astype(
        jnp.bfloat16
    )
    rdim, pdim, adim, mdim = binned.shape
    seg = interp.shape[2]
    gdim = mdim // seg
    side = cos_t.shape[0]
    pieces = binned.reshape(rdim, pdim, adim, gdim, seg)
    contrib = jnp.einsum("rpagj,agjt->rpagt", pieces, interp, preferred_element_type=f32)
    flat = jnp.zeros((rdim, pdim, side * side // seg, seg), f32)
    flat = flat.at[:, :, block_index.reshape(-1)].add(contrib.reshape(rdim, pdim, adim * gdim, seg))
    grid = flat.reshape(rdim, pdim, side, side).astype(jnp.bfloat16)
    half_re = jnp.einsum("ky,pyx->pkx", cos_t, grid[0], preferred_element_type=f32) + jnp.einsum(
        "ky,pyx->pkx", sin_t, grid[1], preferred_element_type=f32
    )
    half_im = jnp.einsum("ky,pyx->pkx", cos_t, grid[1], preferred_element_type=f32) - jnp.einsum(
        "ky,pyx->pkx", sin_t, grid[0], preferred_element_type=f32
    )
    half_re = half_re.astype(jnp.bfloat16)
    half_im = half_im.astype(jnp.bfloat16)
    out_re = jnp.einsum("pkx,mx->pkm", half_re, cos_t, preferred_element_type=f32) + jnp.einsum(
        "pkx,mx->pkm", half_im, sin_t, preferred_element_type=f32
    )
    out_im = jnp.einsum("pkx,mx->pkm", half_im, cos_t, preferred_element_type=f32) - jnp.einsum(
        "pkx,mx->pkm", half_re, sin_t, preferred_element_type=f32
    )
    return jnp.stack([out_re, out_im])


def conj_product(sens, image):
    real_part = sens[0] * image[0] + sens[1] * image[1]
    imag_part = sens[0] * image[1] - sens[1] * image[0]
    return jnp.stack([real_part, imag_part])


def per_device(kdata, spoke_angle, spoke_count, block_index, interp, sens_maps):
    side = sens_maps.shape[2]
    parts_here = kdata.shape[1]
    spokes = kdata.shape[3]
    angles = interp.shape[0]
    cos_t, sin_t = dft_tables(side, jnp.bfloat16)
    position = jnp.arange(spokes, dtype=jnp.int32)
    used = position[None, :] < spoke_count[:, None]
    match = spoke_angle[:, None] == jnp.arange(angles, dtype=jnp.int32)[None, :]
    weights = (used[:, :, None] & match[None, :, :]).astype(jnp.bfloat16)
    data = kdata[:, :, 0]
    image_c = coil_image(data, weights, interp, block_index, cos_t, sin_t)
    sens_here = sens_maps.astype(jnp.float32)
    weighted = conj_product(sens_here[:, 0][:, None], image_c)
    combined = lax.psum_scatter(weighted, "coil", scatter_dimension=2, tiled=True)
    groups = lax.axis_size("kz")
    kz_total = parts_here * groups
    my_first = lax.axis_index("kz") * parts_here
    piece = lax.all_gather(combined, "kz", axis=1, tiled=True)
    cos_z, sin_z = kz_block(my_first, parts_here, piece.shape[1], kz_total)
    return kz_apply(cos_z, sin_z, piece)


def solution(mesh):
    placed = (
        P(None, "kz", "coil", None, None),
        P(),
        P("kz"),
        P(),
        P(),
        P(None, "coil", None, None),
    )
    fast = mesh.shape["coil"] == 8 and mesh.shape["kz"] == 4
    return jax.shard_map(
        fast_device if fast else per_device,
        mesh=mesh,
        in_specs=placed,
        out_specs=P(None, "kz", "coil", None),
        check_vma=False,
    )
```

```python
import functools

import jax
import jax.numpy as jnp
import numpy as np
from jax import lax
from jax.experimental import pallas as pl
from jax.experimental.pallas import tpu as pltpu
from jax.sharding import PartitionSpec as P

ROW_CUTS = 1


def host_tables(length, dtype):
    index = np.arange(length, dtype=np.int32)
    product = index[:, None] * index[None, :] % length
    phase = product.astype(np.float32) * np.float32(2.0 * np.pi / length)
    scale = np.float32(1.0) / np.sqrt(np.float32(length))
    return ((np.cos(phase) * scale).astype(dtype), (np.sin(phase) * scale).astype(dtype))


def store_pieces(out, sens_re, sens_im, send_ref, keep_ref, q):
    nrows, width = out.shape[0], out.shape[1] // 2
    pieces = keep_ref.shape[0]
    sub = nrows // (2 * pieces)
    re, im = out[:, :width], out[:, width:]
    w = (sens_re * re + sens_im * im, sens_re * im - sens_im * re)
    for r in range(2):
        for m in range(pieces):
            keep_ref[m, r, q * sub:(q + 1) * sub, :] = w[r][m * sub:(m + 1) * sub]
            send_ref[m, r, q * sub:(q + 1) * sub, :] = w[r][(pieces + m) * sub:(pieces + m + 1) * sub]


def grid_kernel(
    count_ref, bidx_ref, rows_ref, angle_ref, table_ref, sens_ref, m2_ref, data_ref, interp_hbm,
    half_ref, sensp_ref, send_ref, keep_ref,
    bin_ref, grid_ref, m1_ref, interp_ref, sem,
):
    f32, bf16 = jnp.float32, jnp.bfloat16
    step = pl.program_id(0)
    group = data_ref.shape[1]
    parts = pl.num_programs(0) // 2
    angles, segs = bidx_ref.shape
    seg = interp_ref.shape[1]
    side = table_ref.shape[0]
    spokes = angle_ref.shape[1]
    lines = 2 * bin_ref.shape[1] // (2 * angles)
    nblocks = grid_ref.shape[0] // lines
    per_row = side // seg
    nparts = lines // 2

    @pl.when(step == 0)
    def _():
        pltpu.make_async_copy(interp_hbm, interp_ref, sem).start()
        pick = (lax.broadcasted_iota(jnp.int32, (side, side), 1) == rows_ref[...]).astype(bf16)
        both = jnp.dot(pick, table_ref[...], preferred_element_type=f32)
        pc, ps = both[:, :side], both[:, side:]
        m1_ref[:side, :side] = pc.astype(bf16)
        m1_ref[:side, side:] = ps.astype(bf16)
        m1_ref[side:, :side] = (-ps).astype(bf16)
        m1_ref[side:, side:] = pc.astype(bf16)
        for r in range(2):
            sensp_ref[r] = jnp.dot(pick, sens_ref[r], preferred_element_type=f32)

    @pl.when(step < parts)
    def _():
        zrows = grid_ref.shape[0] // parts
        grid_ref[pl.ds(step * zrows, zrows), :] = jnp.zeros((zrows, seg), f32)
        a_iota = lax.broadcasted_iota(jnp.int32, (angles, spokes), 0)
        s_iota = lax.broadcasted_iota(jnp.int32, (angles, spokes), 1)
        for q in range(group):
            part = step * group + q
            keep = (a_iota == angle_ref[...]) & (s_iota < count_ref[part])
            wt = jnp.where(keep, 1.0, 0.0).astype(bf16)
            for r in range(2):
                b = jnp.dot(wt, data_ref[r, q], preferred_element_type=f32)
                b = b.astype(bf16).astype(f32)
                for g in range(segs):
                    bin_ref[g, pl.ds((r * nparts + part) * angles, angles), :] = b[:, g * seg:(g + 1) * seg]

    @pl.when(step == parts)
    def _():
        pltpu.make_async_copy(interp_hbm, interp_ref, sem).wait()
        unroll = 4 if angles % 4 == 0 else 1

        def body(i, carry):
            res = []
            for u in range(unroll):
                a = i * unroll + u
                for g in range(0, segs, 2):
                    lhs = jnp.concatenate(
                        [bin_ref[g + k, pl.ds(a, lines, stride=angles), :].astype(bf16) for k in range(2)], axis=0
                    )
                    rhs = jnp.concatenate([interp_ref[a * segs + g + k] for k in range(2)], axis=1)
                    both = jnp.dot(lhs, rhs, preferred_element_type=f32)
                    for k in range(2):
                        res.append((bidx_ref[a, g + k], both[k * lines:(k + 1) * lines, k * seg:(k + 1) * seg]))
            for b, v in res:
                at = pl.ds(pl.multiple_of(b * lines, lines), lines)
                grid_ref[at, :] = grid_ref[at, :] + v
            return carry

        lax.fori_loop(0, angles // unroll, body, 0)

    @pl.when(step >= parts)
    def _():
        for q in range(group):
            p = (step - parts) * group + q
            stacked = jnp.concatenate(
                [
                    jnp.concatenate(
                        [
                            grid_ref[pl.ds(h * lines + r * nparts + p, side, stride=per_row * lines), :].astype(bf16)
                            for h in range(per_row)
                        ],
                        axis=1,
                    )
                    for r in range(2)
                ],
                axis=0,
            )
            half = jnp.dot(m1_ref[...], stacked, preferred_element_type=f32).astype(bf16)
            half_ref[q, :, :side] = half[:side]
            half_ref[q, :, side:] = half[side:]
            nrows = side // ROW_CUTS
            width = m2_ref.shape[1] // 2
            both = jnp.concatenate([half[:nrows], half[side:side + nrows]], axis=1)
            out = jnp.dot(both, m2_ref[...], preferred_element_type=f32)
            store_pieces(out, sensp_ref[0, :nrows, :width], sensp_ref[1, :nrows, :width], send_ref, keep_ref, q)


def image_kernel(half_ref, m2_ref, sens_ref, send_ref, keep_ref):
    pp, nrows, depth = half_ref.shape
    out = jnp.dot(half_ref[...].reshape(pp * nrows, depth), m2_ref[...], preferred_element_type=jnp.float32)
    for q in range(pp):
        store_pieces(out[q * nrows:(q + 1) * nrows], sens_ref[0], sens_ref[1], send_ref, keep_ref, q)


def kz_kernel(cnt, z_ref, *refs):
    n = len(refs) // 2
    ins, outs = refs[:n], refs[n:]
    rows, width = ins[0].shape
    sub = rows // (2 * cnt)
    x = jnp.concatenate(
        [
            jnp.concatenate(
                [ins[s][pl.ds(r * cnt * sub + i, cnt, stride=sub), :] for s in range(n) for r in range(2)], axis=0
            )
            for i in range(sub)
        ],
        axis=1,
    )
    y = jnp.dot(z_ref[...], x, preferred_element_type=jnp.float32, precision=lax.Precision.HIGHEST)
    for s in range(n):
        for r in range(2):
            for i in range(sub):
                outs[s][pl.ds(r * cnt * sub + i, cnt, stride=sub), :] = y[
                    (s * 2 + r) * cnt:(s * 2 + r + 1) * cnt, i * width:(i + 1) * width
                ]


def place_kernel(me_ref, *refs):
    out_ref = refs[-1]
    ins = refs[:-1]
    _, cnt, _, side = out_ref.shape
    width = ins[0].shape[1]
    sub = ins[0].shape[0] // (2 * cnt)
    cuts = side // width
    n = len(ins) // (cuts * ROW_CUTS)
    for j in range(cuts):
        for s in range(n):
            at = pl.multiple_of((me_ref[0] ^ s) * (sub * ROW_CUTS), sub * ROW_CUTS)
            for r in range(2):
                for z in range(cnt):
                    k = (r * cnt + z) * sub
                    out_ref[r, z, pl.ds(at, sub * ROW_CUTS), j * width:(j + 1) * width] = jnp.concatenate(
                        [ins[(t * cuts + j) * n + s][k:k + sub, :] for t in range(ROW_CUTS)], axis=0
                    )


def swap(x, axis, bit):
    n = lax.axis_size(axis)
    return lax.ppermute(x, axis, [(i, i ^ bit) for i in range(n)])


def piece_order():
    order = []
    for relc in range(2):
        order += [(relc, 1, ry, rd) for ry in range(2) for rd in (0, 1)]
        order += [(relc, 0, ry, rd) for ry in range(2) for rd in (0, 1)]
        order += [(relc, rx, 1, rd) for rx in range(2) for rd in (2, 3)]
        order += [(relc, rx, 0, rd) for rx in range(2) for rd in (2, 3)]
    coil_rel = np.array([c + 2 * x + 4 * y for c, x, y, d in order], np.int32)
    kz_rel = np.array([d for c, x, y, d in order], np.int32)
    return coil_rel, kz_rel


def fast_device(kdata, spoke_angle, spoke_count, block_index, interp, sens_maps):
    f32, bf16 = jnp.float32, jnp.bfloat16
    _, parts, _, spokes, samples = kdata.shape
    side = sens_maps.shape[2]
    angles, segs, seg, _ = interp.shape
    groups = lax.axis_size("kz")
    mine_c = lax.axis_index("coil")
    mine_d = lax.axis_index("kz")
    full = side // (lax.axis_size("coil") * groups)
    sub = full // ROW_CUTS
    coil_rel, kz_rel = piece_order()
    starts = (mine_c ^ coil_rel) * (full * groups) + (mine_d ^ kz_rel) * full
    offset = np.arange(ROW_CUTS * sub, dtype=np.int32).reshape(ROW_CUTS, 1, sub)
    rows = (starts[None, :, None] + offset).reshape(side, 1)
    cos_h, sin_h = host_tables(side, np.float32)
    table = jnp.asarray(np.concatenate([cos_h, sin_h], 1).astype(bf16))
    lines = 2 * parts
    pp = 8
    steps = parts // pp
    smem = pl.BlockSpec(memory_space=pltpu.SMEM)
    whole = lambda shape: pl.BlockSpec(shape, lambda i: (0,) * len(shape))
    width = 128
    chunks = side // width
    npieces = len(coil_rel) // 2
    nrows = side // ROW_CUTS
    m2s = []
    for j in range(chunks):
        cols = slice(j * width, (j + 1) * width)
        ct, st = cos_h.T[:, cols], sin_h.T[:, cols]
        m2 = np.concatenate([np.concatenate([ct, -st], 1), np.concatenate([st, ct], 1)], 0)
        m2s.append(jnp.asarray(m2.astype(bf16)))
    out_type = jax.ShapeDtypeStruct((npieces, 2, parts * sub, width), f32)
    first_spec = pl.BlockSpec((npieces, 2, pp * sub, width), lambda i: (0, 0, jnp.maximum(i - steps, 0), 0))
    half, sens_p, *first = pl.pallas_call(
        grid_kernel,
        grid=(2 * steps,),
        in_specs=[
            smem, smem, whole((side, 1)), whole((1, spokes)), whole((side, 2 * side)),
            whole((2, side, side)), whole((2 * side, 2 * width)),
            pl.BlockSpec((2, pp, spokes, samples), lambda i: (0, jnp.minimum(i, steps - 1), 0, 0)),
            pl.BlockSpec(memory_space=pl.ANY),
        ],
        out_specs=[
            pl.BlockSpec((pp, side, 2 * side), lambda i: (jnp.maximum(i - steps, 0), 0, 0)),
            whole((2, side, side)), first_spec, first_spec,
        ],
        out_shape=[
            jax.ShapeDtypeStruct((parts, side, 2 * side), bf16),
            jax.ShapeDtypeStruct((2, side, side), f32), out_type, out_type,
        ],
        scratch_shapes=[
            pltpu.VMEM((segs, lines * angles, seg), f32),
            pltpu.VMEM((side * side // seg * lines, seg), f32),
            pltpu.VMEM((2 * side, 2 * side), bf16),
            pltpu.VMEM((angles * segs, seg, seg), bf16),
            pltpu.SemaphoreType.DMA,
        ],
        compiler_params=pltpu.CompilerParams(
            dimension_semantics=("arbitrary",), vmem_limit_bytes=48 * 1024 * 1024
        ),
        name="grid_half",
    )(
        spoke_count, block_index, rows, spoke_angle.reshape(1, spokes), table,
        sens_maps[:, 0], m2s[0], kdata[:, :, 0], interp.reshape(angles * segs, seg, seg),
    )

    flat = 2 * parts * sub
    kz_total = parts * groups
    order = ((mine_d ^ np.arange(groups, dtype=np.int32))[:, None] * parts + np.arange(parts, dtype=np.int32)[None, :])
    prod = order[:, None, :, None] * order[None, :, None, :] % kz_total
    phase = prod.astype(f32) * (2.0 * jnp.pi / kz_total)
    scale = 1.0 / jnp.sqrt(f32(kz_total))
    cz, sz = jnp.cos(phase) * scale, jnp.sin(phase) * scale
    zmat = jnp.stack([jnp.stack([cz, sz], 3), jnp.stack([-sz, cz], 3)], 1)
    zmat = jnp.transpose(zmat, (0, 1, 3, 2, 4, 5)).reshape(2 * kz_total, 2 * kz_total)

    finals = []
    before = None
    for t, j in [(t, j) for t in range(ROW_CUTS) for j in range(chunks)]:
        out_spec = pl.BlockSpec((npieces, 2, pp * sub, width), lambda i: (0, 0, i, 0))
        send, keep = first if t == j == 0 else pl.pallas_call(
            image_kernel,
            grid=(parts // pp,),
            in_specs=[
                pl.BlockSpec((pp, nrows, 2 * side), lambda i, t=t: (i, t, 0)),
                pl.BlockSpec((2 * side, 2 * width), lambda i: (0, 0)),
                pl.BlockSpec((2, nrows, width), lambda i, t=t, j=j: (0, t, j)),
            ],
            out_specs=[out_spec, out_spec],
            out_shape=[out_type, out_type],
            compiler_params=pltpu.CompilerParams(
                dimension_semantics=("arbitrary",), vmem_limit_bytes=48 * 1024 * 1024
            ),
            name="image_piece",
        )(half, m2s[j], sens_p)
        got = swap(send, "coil", 1)
        q = npieces // 4
        h = q // 2
        if before is not None:
            got, *before = lax.optimization_barrier((got, *before))
        x_send = keep[:q] + got[:q]
        y_send = keep[2 * q:3 * q] + got[2 * q:3 * q]
        x_got = swap(x_send, "coil", 2)
        y_got = swap(y_send, "coil", 4)
        x_keep = keep[q:2 * q] + got[q:2 * q]
        y_keep = keep[3 * q:] + got[3 * q:]
        xy_send = x_keep[h:] + x_got[h:]
        yx_send = y_keep[h:] + y_got[h:]
        before = (xy_send, yx_send)
        xy_got = swap(xy_send, "coil", 4)
        yx_got = swap(yx_send, "coil", 2)
        mine = [x_keep[s] + x_got[s] + xy_got[s] for s in range(h)]
        mine += [y_keep[s] + y_got[s] + yx_got[s] for s in range(h)]
        arrived = [mine[0]] + [swap(mine[s], "kz", s) for s in range(1, groups)]
        spun = pl.pallas_call(
            functools.partial(kz_kernel, parts),
            out_shape=[jax.ShapeDtypeStruct((flat, width), f32)] * groups,
            name="kz_dft",
        )(zmat, *[v.reshape(flat, width) for v in arrived])
        finals += [spun[0]] + [swap(spun[s], "kz", s) for s in range(1, groups)]
    vm = pl.BlockSpec(memory_space=pltpu.VMEM)
    return pl.pallas_call(
        place_kernel,
        in_specs=[smem] + [vm] * len(finals),
        out_specs=vm,
        out_shape=jax.ShapeDtypeStruct((2, parts, full * groups, side), f32),
        name="place",
    )(mine_d.reshape(1).astype(jnp.int32), *finals)


def dft_tables(length, dtype):
    index = jnp.arange(length, dtype=jnp.int32)
    product = index[:, None] * index[None, :] % length
    phase = product.astype(jnp.float32) * (2.0 * jnp.pi / length)
    scale = 1.0 / jnp.sqrt(jnp.float32(length))
    return ((jnp.cos(phase) * scale).astype(dtype), (jnp.sin(phase) * scale).astype(dtype))


def kz_block(z_first, z_count, k_count, length):
    z_index = z_first + jnp.arange(z_count, dtype=jnp.int32)
    k_index = jnp.arange(k_count, dtype=jnp.int32)
    product = z_index[:, None] * k_index[None, :] % length
    phase = product.astype(jnp.float32) * (2.0 * jnp.pi / length)
    scale = 1.0 / jnp.sqrt(jnp.float32(length))
    return (jnp.cos(phase) * scale, jnp.sin(phase) * scale)


def kz_apply(cos_z, sin_z, slab):
    high = lax.Precision.HIGHEST
    real_part = jnp.einsum("zk,kyx->zyx", cos_z, slab[0], precision=high) + jnp.einsum(
        "zk,kyx->zyx", sin_z, slab[1], precision=high
    )
    imag_part = jnp.einsum("zk,kyx->zyx", cos_z, slab[1], precision=high) - jnp.einsum(
        "zk,kyx->zyx", sin_z, slab[0], precision=high
    )
    return jnp.stack([real_part, imag_part])


def coil_image(data, weights, interp, block_index, cos_t, sin_t):
    f32 = jnp.float32
    binned = jnp.einsum("rpsn,psa->rpan", data, weights, preferred_element_type=f32).astype(
        jnp.bfloat16
    )
    rdim, pdim, adim, mdim = binned.shape
    seg = interp.shape[2]
    gdim = mdim // seg
    side = cos_t.shape[0]
    pieces = binned.reshape(rdim, pdim, adim, gdim, seg)
    contrib = jnp.einsum("rpagj,agjt->rpagt", pieces, interp, preferred_element_type=f32)
    flat = jnp.zeros((rdim, pdim, side * side // seg, seg), f32)
    flat = flat.at[:, :, block_index.reshape(-1)].add(contrib.reshape(rdim, pdim, adim * gdim, seg))
    grid = flat.reshape(rdim, pdim, side, side).astype(jnp.bfloat16)
    half_re = jnp.einsum("ky,pyx->pkx", cos_t, grid[0], preferred_element_type=f32) + jnp.einsum(
        "ky,pyx->pkx", sin_t, grid[1], preferred_element_type=f32
    )
    half_im = jnp.einsum("ky,pyx->pkx", cos_t, grid[1], preferred_element_type=f32) - jnp.einsum(
        "ky,pyx->pkx", sin_t, grid[0], preferred_element_type=f32
    )
    half_re = half_re.astype(jnp.bfloat16)
    half_im = half_im.astype(jnp.bfloat16)
    out_re = jnp.einsum("pkx,mx->pkm", half_re, cos_t, preferred_element_type=f32) + jnp.einsum(
        "pkx,mx->pkm", half_im, sin_t, preferred_element_type=f32
    )
    out_im = jnp.einsum("pkx,mx->pkm", half_im, cos_t, preferred_element_type=f32) - jnp.einsum(
        "pkx,mx->pkm", half_re, sin_t, preferred_element_type=f32
    )
    return jnp.stack([out_re, out_im])


def conj_product(sens, image):
    real_part = sens[0] * image[0] + sens[1] * image[1]
    imag_part = sens[0] * image[1] - sens[1] * image[0]
    return jnp.stack([real_part, imag_part])


def per_device(kdata, spoke_angle, spoke_count, block_index, interp, sens_maps):
    side = sens_maps.shape[2]
    parts_here = kdata.shape[1]
    spokes = kdata.shape[3]
    angles = interp.shape[0]
    cos_t, sin_t = dft_tables(side, jnp.bfloat16)
    position = jnp.arange(spokes, dtype=jnp.int32)
    used = position[None, :] < spoke_count[:, None]
    match = spoke_angle[:, None] == jnp.arange(angles, dtype=jnp.int32)[None, :]
    weights = (used[:, :, None] & match[None, :, :]).astype(jnp.bfloat16)
    data = kdata[:, :, 0]
    image_c = coil_image(data, weights, interp, block_index, cos_t, sin_t)
    sens_here = sens_maps.astype(jnp.float32)
    weighted = conj_product(sens_here[:, 0][:, None], image_c)
    combined = lax.psum_scatter(weighted, "coil", scatter_dimension=2, tiled=True)
    groups = lax.axis_size("kz")
    kz_total = parts_here * groups
    my_first = lax.axis_index("kz") * parts_here
    piece = lax.all_gather(combined, "kz", axis=1, tiled=True)
    cos_z, sin_z = kz_block(my_first, parts_here, piece.shape[1], kz_total)
    return kz_apply(cos_z, sin_z, piece)


def solution(mesh):
    placed = (
        P(None, "kz", "coil", None, None),
        P(),
        P("kz"),
        P(),
        P(),
        P(None, "coil", None, None),
    )
    fast = mesh.shape["coil"] == 8 and mesh.shape["kz"] == 4
    return jax.shard_map(
        fast_device if fast else per_device,
        mesh=mesh,
        in_specs=placed,
        out_specs=P(None, "kz", "coil", None),
        check_vma=False,
    )
```
